16 devices in a mesh: col: 2 (over z), row: 8 (over y, x, core).
Axes of the slice: x: 2, y: 2, z: 2, core: 2. Of those that a mesh axis runs over, the one named last changes fastest.
Arguments:
- matrix: bfloat16 [16384, 16384], P('row', 'col')
- y_start: float32 [16384, 128], P(('col', 'row'))
- center: float32 [], replicated
- half_width: float32 [], replicated
Outputs:
- output 1: float32 [16384, 128], P(('col', 'row'))
- output 2: float32 [128, 128], replicated
All inputs are finite; a program needn't handle non-finite values.
Results may differ from the reference program's by a relative error of at most 0.0143295.
Values are sent between devices in bfloat16 or wider.
A program may use at most 1 GiB of HBM per device.

```python
import jax
import jax.numpy as jnp
from jax import lax

N = 16384
WIDTH = 128
DEGREE = 8


def setup_inputs(seed: int = 0) -> dict:
    root_key = jax.random.key(seed)
    key_mat, key_vec, key_center, key_width = jax.random.split(root_key, 4)
    base_draw = jax.random.normal(key_mat, (N, N), jnp.float32)
    matrix = ((base_draw + base_draw.T) * (2.0 * N) ** -0.5).astype(jnp.bfloat16)
    y_start = jax.random.normal(key_vec, (N, WIDTH), jnp.float32)
    center = jax.random.uniform(key_center, (), jnp.float32, -0.5, 0.5)
    half_width = 2.3 + jnp.abs(center) + jax.random.uniform(key_width, (), jnp.float32, 0.0, 0.5)
    return {"matrix": matrix, "y_start": y_start, "center": center, "half_width": half_width}


def apply_matrix(matrix, vectors):
    return jnp.dot(matrix, vectors.astype(jnp.bfloat16), preferred_element_type=jnp.float32)


def reference(matrix, y_start, center, half_width):
    y_first = (apply_matrix(matrix, y_start) - center * y_start) / half_width

    def sweep_step(state_pair, unused):
        y_prev, y_cur = state_pair
        y_next = 2.0 * (apply_matrix(matrix, y_cur) - center * y_cur) / half_width - y_prev
        return (y_cur, y_next), unused

    final_pair, unused_out = lax.scan(sweep_step, (y_start, y_first), None, length=DEGREE - 1)
    y_last = final_pair[1]
    y_low = y_last.astype(jnp.bfloat16)
    image_low = apply_matrix(matrix, y_last).astype(jnp.bfloat16)
    gram_mat = jnp.dot(y_low.T, image_low, preferred_element_type=jnp.float32) / N
    return y_last, gram_mat
```

```python
import jax
import jax.numpy as jnp
from jax import lax
from jax.experimental import pallas as pl
from jax.experimental.pallas import tpu as pltpu
from jax.sharding import PartitionSpec as P

DEGREE = 8
W = 128
CH = 128
NC = 8
NM = 8
ROWS = 2048
COLS = 8192
PAN = 128
NPAN = ROWS // PAN
NST = 4
RB = 256
NT = (((1,), (1,)), ((), ()))
MESH = pl.DeviceIdType.MESH


def kernel(a_hbm, y_in, cen_ref, wid_ref, y_out, g_out,
           at, st, yg, part, xbuf, ycur, yprev, ysend, ystage, gacc, gbuf,
           a_sem, gr, gs, xr, xs, ss, y0r, y0s, yor, yos, rr, rs, ar, as_):
    i = lax.axis_index("row")
    z = lax.axis_index("col")
    c = lax.rem(i, 2)
    x = lax.rem(i // 2, 2)
    y = i // 4
    oc, ox, oy, oz = 1 - c, 1 - x, 1 - y, 1 - z
    flat = z * 8 + i
    aligned = y == z
    crossed = y != z

    def dev(xx, yy, zz, cc):
        return (zz, yy * 4 + xx * 2 + cc)

    plane = [dev(ox, y, z, c), dev(x, oy, z, c), dev(ox, oy, z, c)]
    twin = dev(x, y, z, oc)

    def slot(xx, yy, cc):
        return (xx * 2 + cc) * 2 + yy

    def slot0(xx, yy, cc):
        return yy * 4 + xx * 2 + cc

    def sources(fn):
        mine = fn(x, y, c)
        direct = [fn(ox, y, c), fn(x, oy, c), fn(ox, oy, c)]
        relayed = [fn(xx, yy, oc) for xx in (x, ox) for yy in (y, oy)]
        return mine, direct, relayed

    def load(p):
        return pltpu.make_async_copy(a_hbm.at[pl.ds(p * PAN, PAN), :], st.at[p % NST], a_sem.at[p % NST])

    def rcopy(src, dst, ssem, rsem, device):
        return pltpu.make_async_remote_copy(src_ref=src, dst_ref=dst, send_sem=ssem, recv_sem=rsem,
                                            device_id=device, device_id_type=MESH)

    def push(par, m, k, device):
        ref = yg.at[par, m, k]
        rcopy(ref, ref, gs.at[par], gr.at[par, m, k], device).start()

    def arrived(par, m, k):
        ref = yg.at[par, m, k]
        rcopy(ref, ref, gs.at[par], gr.at[par, m, k], twin).wait_recv()

    def distribute(par, m, k):
        for d in plane:
            push(par, m, k, d)
        push(par, m, k, twin)

    def sent(par):
        pltpu.make_async_copy(yg.at[par, pl.ds(0, 7)], yg.at[par, pl.ds(0, 7)], gs.at[par]).wait()

    for p in range(NST - 1):
        load(p).start()

    barrier = pltpu.get_barrier_semaphore()
    for d in range(1, 16):
        t = lax.rem(flat + d, 16)
        pl.semaphore_signal(barrier, inc=1, device_id=(t // 8, lax.rem(t, 8)), device_id_type=MESH)
    pl.semaphore_wait(barrier, 15)

    mine0, direct0, relayed0 = sources(slot0)
    for k in range(NC):
        t32 = y_in[k * CH:(k + 1) * CH, :].T
        ystage[k] = t32
        yg[0, mine0, k] = t32.astype(jnp.bfloat16)
        distribute(0, mine0, k)
    home = (lax.rem(flat, 2), flat // 2)
    stays = (home[0] == z) & (home[1] == i)
    y0_copy = rcopy(ystage, ycur, y0s, y0r, home)

    @pl.when(stays)
    def _():
        ycur[...] = ystage[...]

    @pl.when(jnp.logical_not(stays))
    def _():
        y0_copy.start()
    yprev[...] = jnp.zeros_like(yprev)

    for p in range(NPAN):
        if p + NST - 1 < NPAN:
            load(p + NST - 1).start()
        load(p).wait()
        for q in range(8):
            at[q * 1024:(q + 1) * 1024, p * PAN:(p + 1) * PAN] = st[p % NST, :, q * 1024:(q + 1) * 1024].T
        k = p - (NPAN - NC)
        if k >= 0:
            for m in direct0:
                arrived(0, m, k)
                push(0, m, k, twin)
    for k in range(NC):
        for m in relayed0:
            arrived(0, m, k)

    def xsend(par, k):
        return rcopy(part.at[par, oz, k], xbuf.at[par, k], xs.at[par], xr.at[par, k], dev(x, y, oz, c))

    def xsent(par):
        pltpu.make_async_copy(part.at[par, 0], part.at[par, 0], xs.at[par]).wait()

    def granule(par, cc, first, last):
        lhs = jnp.concatenate([yg[par, m, cc] for m in range(NM)], axis=1)
        for half in range(2):
            h = oz if half == 0 else z
            for q in range(1024 // RB):
                lanes = pl.ds(pl.multiple_of(h * 1024 + q * RB, RB), RB)
                rhs = jnp.concatenate([at[m * 1024 + cc * CH:m * 1024 + (cc + 1) * CH, lanes] for m in range(NM)], axis=0)
                res = jnp.dot(lhs, rhs, preferred_element_type=jnp.float32)
                for s in range(RB // CH):
                    k = q * (RB // CH) + s
                    val = res[:, s * CH:(s + 1) * CH]
                    if first:
                        part[par, h, k] = val
                    else:
                        part[par, h, k] = part[par, h, k] + val
                    if last and half == 0:
                        xsend(par, k).start()

    for cc in range(NC):
        granule(0, cc, cc == 0, cc == NC - 1)

    @pl.when(jnp.logical_not(stays))
    def _():
        y0_copy.wait()

    mine, direct, relayed = sources(slot)
    swap_to = dev(x, oy, oz, c)
    swap_slot = slot(x, oy, c)

    def summed(par, k):
        rcopy(part.at[par, oz, k], xbuf.at[par, k], xs.at[par], xr.at[par, k], dev(x, y, oz, c)).wait_recv()
        return part[par, z, k] + xbuf[par, k]

    def body(t, carry):
        par = lax.rem(t, 2)
        nxt = 1 - par
        center = cen_ref[0]
        width = wid_ref[0]
        scale = jnp.where(t == 0, 1.0, 2.0).astype(jnp.float32)
        keep = jnp.where(t == 0, 0.0, 1.0).astype(jnp.float32)

        def advance(k):
            total = summed(par, k)
            old = ycur[k]
            new = scale * (total - center * old) / width - keep * yprev[k]
            yprev[k] = old
            ycur[k] = new
            low = new.astype(jnp.bfloat16)

            @pl.when(aligned)
            def _():
                yg[nxt, mine, k] = low
                distribute(nxt, mine, k)

            @pl.when(crossed)
            def _():
                ysend[nxt, k] = low
                rcopy(ysend.at[nxt, k], yg.at[nxt, swap_slot, k], ss.at[nxt], gr.at[nxt, swap_slot, k], swap_to).start()

        def spread(k):
            @pl.when(crossed)
            def _():
                arrived(nxt, mine, k)
                distribute(nxt, mine, k)

        def relay(k):
            for m in direct:
                arrived(nxt, m, k)
                push(nxt, m, k, twin)

        sent(par)
        for step in range(NC + 3):
            if step < NC:
                advance(step)
            if 0 <= step - 1 < NC:
                spread(step - 1)
            if 0 <= step - 2 < NC:
                relay(step - 2)
            if 0 <= step - 3 < NC:
                k = step - 3
                for m in relayed:
                    arrived(nxt, m, k)
                granule(nxt, k, k == 0, k == NC - 1)
        xsent(par)

        @pl.when(crossed)
        def _():
            pltpu.make_async_copy(ysend.at[nxt], ysend.at[nxt], ss.at[nxt]).wait()
        return carry

    lax.fori_loop(0, DEGREE, body, 0)
    last = DEGREE % 2

    q = i * 2 + z
    place = (q // 8, lax.rem(q, 8))
    ends_here = (place[0] == z) & (place[1] == i)
    for k in range(NC):
        ystage_rows = ycur[k].T
        ystage[k] = ystage_rows
    out_copy = rcopy(ystage, y_out, yos, yor, place)

    @pl.when(ends_here)
    def _():
        y_out[...] = ystage[...]

    @pl.when(jnp.logical_not(ends_here))
    def _():
        out_copy.start()

    for k in range(NC):
        image = summed(last, k).astype(jnp.bfloat16)
        term = lax.dot_general(ycur[k].astype(jnp.bfloat16), image, NT, preferred_element_type=jnp.float32)
        if k == 0:
            gacc[...] = term
        else:
            gacc[...] += term
    xsent(last)
    sent(last)

    def ring(d):
        t = lax.rem(flat + d, 16)
        return t, (t // 8, lax.rem(t, 8))

    def rs_copy(d):
        t, device = ring(d)
        return rcopy(gacc.at[pl.ds(pl.multiple_of(t * 8, 8), 8), :], gbuf.at[d], rs.at[d], rr.at[d], device)

    for d in range(1, 16):
        rs_copy(d).start()
    own = pl.ds(pl.multiple_of(flat * 8, 8), 8)
    total = gacc[own, :]
    for d in range(1, 16):
        rs_copy(d).wait_recv()
        total = total + gbuf[d]
    g_out[own, :] = total * (1.0 / 16384)

    def ag_copy(d):
        return rcopy(g_out.at[own, :], g_out.at[own, :], as_.at[d], ar.at[d], ring(d)[1])

    for d in range(1, 16):
        ag_copy(d).start()
    for d in range(1, 16):
        ag_copy(d).wait()
        rs_copy(d).wait_send()

    @pl.when(jnp.logical_not(ends_here))
    def _():
        out_copy.wait()


def solution(mesh):
    both = ("col", "row")
    f32, bf16 = jnp.float32, jnp.bfloat16
    dma = pltpu.SemaphoreType.DMA
    vmem = pl.BlockSpec(memory_space=pltpu.VMEM)
    smem = pl.BlockSpec(memory_space=pltpu.SMEM)

    def local(mat_tile, y_start, center, half_width):
        y, g = pl.pallas_call(
            kernel,
            out_shape=(jax.ShapeDtypeStruct((NC, CH, W), f32), jax.ShapeDtypeStruct((W, W), f32)),
            in_specs=[pl.BlockSpec(memory_space=pl.ANY), vmem, smem, smem],
            out_specs=(vmem, vmem),
            scratch_shapes=[
                pltpu.VMEM((COLS, ROWS), bf16),
                pltpu.VMEM((NST, PAN, COLS), bf16),
                pltpu.VMEM((2, NM, NC, W, CH), bf16),
                pltpu.VMEM((2, 2, NC, W, CH), f32),
                pltpu.VMEM((2, NC, W, CH), f32),
                pltpu.VMEM((NC, W, CH), f32),
                pltpu.VMEM((NC, W, CH), f32),
                pltpu.VMEM((2, NC, W, CH), bf16),
                pltpu.VMEM((NC, W, CH), f32),
                pltpu.VMEM((W, W), f32),
                pltpu.VMEM((16, 8, W), f32),
                dma((NST,)),
                dma((2, NM, NC)),
                dma((2,)),
                dma((2, NC)),
                dma((2,)),
                dma((2,)),
                dma, dma, dma, dma,
                dma((16,)), dma((16,)), dma((16,)), dma((16,)),
            ],
            compiler_params=pltpu.CompilerParams(collective_id=0, has_side_effects=True, vmem_limit_bytes=67043328),
            name="chebyshev",
        )(mat_tile, y_start, center.reshape(1), half_width.reshape(1))
        return y.reshape(NC * CH, W), g

    return jax.shard_map(local, mesh=mesh, in_specs=(P("row", "col"), P(both, None), P(), P()),
                         out_specs=(P(both, None), P()), check_vma=False)
```
